512 devices in a mesh: ctx: 128 (over z, x, y_hi), head: 4 (over y_lo, core).
Axes of the slice: x: 4, y: 4 (y_hi: 2, y_lo: 2; y = y_hi * 2 + y_lo), z: 16, core: 2. Of those that a mesh axis runs over, the one named last changes fastest.
Arguments:
- queries: bfloat16 [8192, 8192], P('ctx', 'head'), may hold values from -6 to 6
- keys: bfloat16 [8192, 128], P('ctx'), may hold values from -6 to 6
- key_gain: float32 [128], replicated, may hold values from 0.25 to 1.75
- key_bias: float32 [128], replicated, may hold values from -0.5 to 0.5
- head_weights: bfloat16 [8192, 64], P('ctx', 'head'), may hold values from -6 to 6
- positions: int32 [8192], P('ctx'), may hold values from 0 to 6143, as said below
Outputs:
- index_scores: float32 [8192, 8192], P(('ctx', 'head'))
The draws below stay inside these ranges and needn't reach their ends.
Inputs may be any that keep to these rules, and one draw needn't show every extreme that they name: `positions`: positions of packed documents: the first 6144 tokens form one document and the rest is split into one to three documents at drawn points; a token's position counts from its document's first token.
All inputs are finite; a program needn't handle non-finite values.
Results may differ from the reference program's by a relative error of at most 0.0095.
Values may be sent and summed in bfloat16 or wider, within the bound.
No kernel may reach another device: no remote copies, remote signals or barrier semaphores. Data moves between devices by JAX's collectives and lax.ppermute only.
A program may use at most 64 MiB of HBM per device.

```python
import math
import jax
import jax.numpy as jnp
import numpy as np
from jax import lax

H = 64
DH = 128
ROPE = 64
TOKENS = 8192
N_HEAD = 4


def draw_positions(key, part):
    first_end = 3 * TOKENS // 4
    cuts = jax.random.randint(key, (2,), first_end + 1, TOKENS)
    token_ids = jnp.arange(TOKENS, dtype=jnp.int32)
    starts = jnp.where(token_ids >= first_end, first_end, 0).astype(jnp.int32)
    starts = jnp.where(token_ids >= cuts[0], jnp.maximum(starts, cuts[0]), starts)
    starts = jnp.where(token_ids >= cuts[1], jnp.maximum(starts, cuts[1]), starts)
    return (token_ids - starts).astype(jnp.int32)


def level_of(rng, dims, cuts, low, largest):
    def one(position, shards_of):
        steps = jax.random.uniform(jax.random.fold_in(jax.random.fold_in(rng, 6), position), (shards_of,), jnp.float32, low / len(cuts), largest / len(cuts))
        return jnp.repeat(jnp.exp(steps), dims[position] // shards_of).reshape((-1,) + (1,) * (len(dims) - position - 1))

    factor_of = one(*cuts[0])
    for cut in cuts[1:]:
        factor_of = factor_of * one(*cut)
    return factor_of


def normal_values(own_key, shape, scale, reach, split=(), kind=jnp.bfloat16):
    values = jax.random.normal(own_key, shape, jnp.float32) * scale
    if len(split) > 0:
        values = level_of(own_key, shape, split, -0.22, 0.18) * values
    return jnp.clip(values, min=-reach, max=reach).astype(kind)


def setup_inputs(seed: int = 0) -> dict:
    key_list = jax.random.split(jax.random.key(seed), 7)
    queries = normal_values(key_list[0], (TOKENS, H * DH), 1.0, 6.0, ((0, 128), (1, 4)))
    keys = normal_values(key_list[1], (TOKENS, DH), 1.0, 6.0, ((0, 128),))
    key_gain = jnp.clip(1.0 + 0.15 * jax.random.normal(key_list[2], (DH,), jnp.float32), 0.25, 1.75)
    key_bias = jnp.clip(jax.random.uniform(key_list[3], (DH,), jnp.float32, -0.5, 0.5), -0.5, 0.5)
    head_weights = normal_values(key_list[4], (TOKENS, H), 1.0, 6.0, ((0, 128), (1, 4)))
    positions = draw_positions(jax.random.fold_in(key_list[6], 71), 0)
    return {"queries": queries, "keys": keys, "key_gain": key_gain, "key_bias": key_bias, "head_weights": head_weights, "positions": positions}


def yarn_frequencies(rope_dims):
    half_dims = rope_dims // 2
    exponent = np.arange(0, rope_dims, 2) / rope_dims
    extra_freq = 1.0 / 10000.0 ** exponent
    inter_freq = extra_freq / 40.0

    def correction(beta):
        return rope_dims * math.log(4096.0 / (beta * 2.0 * math.pi)) / (2.0 * math.log(10000.0))
    low_dim = max(math.floor(correction(32.0)), 0)
    high_dim = min(math.ceil(correction(1.0)), rope_dims - 1)
    if high_dim == low_dim:
        high_dim = high_dim + 0.001
    ramp_values = np.clip((np.arange(half_dims) - low_dim) / (high_dim - low_dim), 0.0, 1.0)
    return (inter_freq * ramp_values + extra_freq * (1.0 - ramp_values)).astype(np.float32)

def rotate(values, angles):
    half_rope = ROPE // 2
    cosine = jnp.cos(angles)[:, None, :]
    sine = jnp.sin(angles)[:, None, :]
    first = values[..., :half_rope]
    second = values[..., half_rope:ROPE]
    return jnp.concatenate([first * cosine - second * sine, second * cosine + first * sine, values[..., ROPE:]], -1)

def key_norm(keys, key_gain, key_bias):
    values = keys.astype(jnp.float32)
    centered = values - lax.optimization_barrier(jnp.mean(values, axis=-1, keepdims=True))
    spread = lax.optimization_barrier(jnp.mean(centered * centered, axis=-1, keepdims=True))
    return centered * lax.rsqrt(spread + 1e-06) * key_gain + key_bias

def tile_scores(q_block, weights, k_block, groups, row_glob, row_doc, key_glob):
    rows_here = q_block.shape[0]
    heads_here = weights.shape[1]
    raw = lax.dot_general(q_block.reshape(rows_here * heads_here, DH), k_block, (((1,), (1,)), ((), ())), preferred_element_type=jnp.float32)
    active = jnp.maximum(raw, 0.0).reshape(rows_here, groups, heads_here // groups, k_block.shape[0])
    partial_sum = lax.optimization_barrier(jnp.sum(active * weights.reshape(rows_here, groups, heads_here // groups, 1), axis=2))
    visible = (key_glob[None, :] >= row_doc[:, None]) & (key_glob[None, :] <= row_glob[:, None])
    partial_sum = jnp.where(visible[:, None, :], partial_sum, jnp.zeros_like(partial_sum))
    return partial_sum.astype(jnp.bfloat16)

def reference(queries, keys, key_gain, key_bias, head_weights, positions):
    freqs = jnp.asarray(yarn_frequencies(ROPE))
    angles = positions.astype(jnp.float32)[:, None] * freqs[None, :]
    q_rot = rotate(queries.astype(jnp.float32).reshape(TOKENS, H, DH), angles).reshape(TOKENS, H * DH).astype(jnp.bfloat16)
    k_rot = rotate(key_norm(keys, key_gain, key_bias)[:, None, :], angles).reshape(TOKENS, DH).astype(jnp.bfloat16)
    weights = head_weights.astype(jnp.float32) * (1.0 / math.sqrt(H * DH))
    token_ids = jnp.arange(TOKENS, dtype=jnp.int32)
    doc_start = token_ids - positions
    block_len = math.gcd(TOKENS, 512)
    block_count = TOKENS // block_len

    def query_block(q_index):
        row_first = (q_index * block_len).astype(jnp.int32)
        q_block = lax.dynamic_slice_in_dim(q_rot, row_first, block_len, 0)
        w_block = lax.dynamic_slice_in_dim(weights, row_first, block_len, 0)
        row_glob = lax.dynamic_slice_in_dim(token_ids, row_first, block_len, 0)
        row_doc = lax.dynamic_slice_in_dim(doc_start, row_first, block_len, 0)

        def key_block(k_index):
            key_first = (k_index * block_len).astype(jnp.int32)
            k_block = lax.dynamic_slice_in_dim(k_rot, key_first, block_len, 0)
            key_glob = key_first + jnp.arange(block_len, dtype=jnp.int32)
            live = (key_first <= jnp.max(row_glob)) & (key_first + block_len > jnp.min(row_doc))

            def compute(operand):
                parts = tile_scores(q_block, w_block, k_block, N_HEAD, row_glob, row_doc, key_glob)
                return lax.optimization_barrier(jnp.sum(parts.astype(jnp.float32), axis=1))

            def skip(operand):
                return jnp.zeros((block_len, block_len), jnp.float32)
            return lax.cond(live, compute, skip, 0)
        tiles = lax.map(key_block, jnp.arange(block_count, dtype=jnp.int32))
        return jnp.transpose(tiles, (1, 0, 2)).reshape(block_len, TOKENS)
    result = lax.map(query_block, jnp.arange(block_count, dtype=jnp.int32))
    return result.reshape(TOKENS, TOKENS)
```

```python
import math

import jax
import jax.numpy as jnp
import numpy as np
from jax import lax
from jax.experimental import pallas as pl
from jax.experimental.pallas import tpu as pltpu
from jax.sharding import Mesh
from jax.sharding import PartitionSpec as P

H = 64
DH = 128
ROPE = 64
ROWS = 64
SUB = 16
HG = 16
QW = HG * DH
PEERS = 32
SLOTS = 3
NK = PEERS * SUB
PLANE = 512
GROUP = 4 * PLANE
SCALE = 1.0 / math.sqrt(H * DH)


def yarn_frequencies(rope_dims):
    half_dims = rope_dims // 2
    exponent = np.arange(0, rope_dims, 2) / rope_dims
    extra_freq = 1.0 / 10000.0**exponent
    inter_freq = extra_freq / 40.0

    def correction(beta):
        return rope_dims * math.log(4096.0 / (beta * 2.0 * math.pi)) / (2.0 * math.log(10000.0))

    low_dim = max(math.floor(correction(32.0)), 0)
    high_dim = min(math.ceil(correction(1.0)), rope_dims - 1)
    ramp_values = np.clip((np.arange(half_dims) - low_dim) / (high_dim - low_dim), 0.0, 1.0)
    return (inter_freq * ramp_values + extra_freq * (1.0 - ramp_values)).astype(np.float32)


def lane_frequencies():
    f = yarn_frequencies(ROPE)
    return np.concatenate([f, f, np.zeros(DH - ROPE, np.float32)])[None, :]


def turn(x, cosine, sine):
    lane = lax.broadcasted_iota(jnp.int32, x.shape, 1)
    half = ROPE // 2
    other = jnp.where(lane < half, pltpu.roll(x, DH - half, 1), pltpu.roll(x, half, 1))
    return x * cosine + other * sine


def cos_sin(pos, freq):
    angle = pos * freq
    lane = lax.broadcasted_iota(jnp.int32, angle.shape, 1)
    sine = jnp.sin(angle)
    return jnp.cos(angle), jnp.where(lane < ROPE // 2, -sine, sine)


def column(row, n, shift):
    m = row.shape[1]
    at = lax.broadcasted_iota(jnp.int32, (n, m), 0) + shift
    lane = lax.broadcasted_iota(jnp.int32, (n, m), 1)
    return jnp.sum(jnp.where(at == lane, jnp.broadcast_to(row, (n, m)), 0.0), axis=1, keepdims=True)


def key_kernel(ids, own, prev, prev2, gain, bias, pos, freq, out):
    head, first = ids[0], ids[1]
    off = head * SUB
    own_pos = column(pos[...].astype(jnp.float32), SUB, off)
    tok = (lax.broadcasted_iota(jnp.int32, (SUB, 1), 0) + (first + off)).astype(jnp.float32)
    for slot, ref in enumerate((own, prev, prev2)):
        v = ref[...].astype(jnp.float32)
        c = v - jnp.mean(v, axis=-1, keepdims=True)
        s = jnp.mean(c * c, axis=-1, keepdims=True)
        k = c * lax.rsqrt(s + 1e-06) * gain[...] + bias[...]
        p = own_pos if slot == 0 else tok - float(slot * GROUP)
        cosine, sine = cos_sin(p, freq[...])
        r = turn(k, cosine, sine).astype(jnp.bfloat16)
        for d in range(PEERS):
            out[d, slot] = r


def query_kernel(q, w, pos, freq, out):
    cosine, sine = cos_sin(column(pos[...].astype(jnp.float32), ROWS, 0), freq[...])
    for h in range(HG):
        x = q[:, h * DH : (h + 1) * DH].astype(jnp.float32)
        out[:, h * DH : (h + 1) * DH] = turn(x, cosine, sine).astype(jnp.bfloat16)
    out[:, QW : QW + HG] = w[...]


def score_kernel(ids, q0, q1, q2, q3, k, pos, out):
    head, first, group = ids[0], ids[1], ids[2]
    row = lax.broadcasted_iota(jnp.int32, (ROWS, 1), 0) + first
    doc = row - column(pos[...].astype(jnp.float32), ROWS, 0).astype(jnp.int32)

    def one(slot, carry):
        kk = k[:, slot].reshape(NK, DH)
        acc = jnp.zeros((ROWS, NK), jnp.float32)
        for q in (q0, q1, q2, q3):
            w = q[:, QW : QW + HG].astype(jnp.float32)
            for h in range(HG):
                s = lax.dot_general(
                    q[:, h * DH : (h + 1) * DH], kk, (((1,), (1,)), ((), ())),
                    preferred_element_type=jnp.float32,
                )
                acc = acc + jnp.maximum(s, 0.0) * w[:, h : h + 1]
        n = lax.broadcasted_iota(jnp.int32, (1, NK), 1)
        key = (group - slot) * GROUP + (n // DH) * PLANE + ((n % DH) // SUB) * ROWS + head * SUB + n % SUB
        seen = (key >= doc) & (key <= row)
        out[:, slot] = jnp.where(seen, acc * SCALE, 0.0).astype(jnp.bfloat16).reshape(4, SUB, NK)
        return carry

    live = jnp.where(group == 3, 1, group + 1)
    for slot in range(SLOTS):
        @pl.when(slot < live)
        def _():
            one(slot, 0)

        @pl.when(slot >= live)
        def _():
            out[:, slot] = jnp.zeros((4, SUB, NK), jnp.bfloat16)


def place_kernel(ids, parts, out):
    group = ids[2]
    out[...] = jnp.zeros_like(out)
    r = lax.broadcasted_iota(jnp.int32, (DH, PLANE), 0)
    c = lax.broadcasted_iota(jnp.int32, (DH, PLANE), 1)
    spread = [
        jnp.where(c == (r // SUB) * ROWS + j * SUB + r % SUB, 1.0, 0.0).astype(jnp.bfloat16)
        for j in range(4)
    ]
    live = jnp.where(group == 3, 1, group + 1)
    for slot in range(SLOTS):
        @pl.when(slot < live)
        def _():
            for z in range(4):
                full = jnp.zeros((SUB, PLANE), jnp.float32)
                for j in range(4):
                    full += jnp.dot(
                        parts[j, slot, :, z * DH : (z + 1) * DH], spread[j],
                        preferred_element_type=jnp.float32,
                    )
                at = pl.multiple_of((group - slot) * GROUP + z * PLANE, PLANE)
                out[:, pl.ds(at, PLANE)] = full


SMEM = pl.BlockSpec(memory_space=pltpu.SMEM)
VMEM = pl.BlockSpec(memory_space=pltpu.VMEM)


def call(kernel, shape, dtype, n, name):
    return pl.pallas_call(
        kernel,
        out_shape=jax.ShapeDtypeStruct(shape, dtype),
        in_specs=[SMEM] * (1 if name != "rotate_queries" else 0) + [VMEM] * n,
        out_specs=VMEM,
        name=name,
    )


def on_device(queries, keys, key_gain, key_bias, head_weights, positions):
    head = lax.axis_index(("yl", "core"))
    ctx = lax.axis_index(("zh", "zl", "x", "yh"))
    group = lax.axis_index("zh")
    ids = jnp.stack([head, ctx * ROWS, group]).astype(jnp.int32)
    freq = jnp.asarray(lane_frequencies())
    pos = positions.reshape(1, ROWS)

    own = lax.dynamic_slice_in_dim(keys, head * SUB, SUB, 0)
    prev = lax.ppermute(own, "zh", [(0, 1), (1, 2)])
    prev2 = lax.ppermute(own, "zh", [(0, 2)])
    sent = call(key_kernel, (PEERS, SLOTS, SUB, DH), jnp.bfloat16, 7, "prepare_keys")(
        ids, own, prev, prev2, key_gain.reshape(1, DH), key_bias.reshape(1, DH), pos, freq
    )
    k_all = lax.all_to_all(sent, ("zl", "x", "yh"), 0, 0, tiled=True)

    q0 = call(query_kernel, (ROWS, QW + DH), jnp.bfloat16, 4, "rotate_queries")(
        queries, head_weights, pos, freq
    )
    swap = [(0, 1), (1, 0)]
    q1 = lax.ppermute(q0, "yl", swap)
    q2 = lax.ppermute(q0, "core", swap)
    q3 = lax.ppermute(q1, "core", swap)

    parts = call(score_kernel, (4, SLOTS, SUB, NK), jnp.bfloat16, 6, "scores")(
        ids, q0, q1, q2, q3, k_all, pos
    )
    parts = lax.all_to_all(parts, ("yl", "core"), 0, 0, tiled=True)
    return call(place_kernel, (SUB, 8192), jnp.float32, 1, "place")(ids, parts)


def solution(mesh):
    names = ("zh", "zl", "x", "yh", "yl", "core")
    fine = Mesh(mesh.devices.reshape(4, 4, 4, 2, 2, 2), names)
    ctx, head = names[:4], names[4:]
    in_specs = (P(ctx, head), P(ctx, None), P(), P(), P(ctx, head), P(ctx))
    return jax.shard_map(
        on_device, mesh=fine, in_specs=in_specs, out_specs=P(names, None), check_vma=False
    )
```

```python
import math

import jax
import jax.numpy as jnp
import numpy as np
from jax import lax
from jax.experimental import pallas as pl
from jax.experimental.pallas import tpu as pltpu
from jax.sharding import Mesh
from jax.sharding import PartitionSpec as P

H = 64
DH = 128
ROPE = 64
ROWS = 64
SUB = 16
HG = 16
QT = HG * ROWS
PEERS = 32
SLOTS = 3
NK = PEERS * SUB
PLANE = 512
GROUP = 4 * PLANE
SCALE = 1.0 / math.sqrt(H * DH)


def yarn_frequencies(rope_dims):
    half_dims = rope_dims // 2
    exponent = np.arange(0, rope_dims, 2) / rope_dims
    extra_freq = 1.0 / 10000.0**exponent
    inter_freq = extra_freq / 40.0

    def correction(beta):
        return rope_dims * math.log(4096.0 / (beta * 2.0 * math.pi)) / (2.0 * math.log(10000.0))

    low_dim = max(math.floor(correction(32.0)), 0)
    high_dim = min(math.ceil(correction(1.0)), rope_dims - 1)
    ramp_values = np.clip((np.arange(half_dims) - low_dim) / (high_dim - low_dim), 0.0, 1.0)
    return (inter_freq * ramp_values + extra_freq * (1.0 - ramp_values)).astype(np.float32)


def lane_frequencies():
    f = yarn_frequencies(ROPE)
    return np.concatenate([f, f, np.zeros(DH - ROPE, np.float32)])[None, :]


def turn(x, cosine, sine):
    lane = lax.broadcasted_iota(jnp.int32, x.shape, 1)
    half = ROPE // 2
    other = jnp.where(lane < half, pltpu.roll(x, DH - half, 1), pltpu.roll(x, half, 1))
    return x * cosine + other * sine


def cos_sin(pos, freq):
    angle = pos * freq
    lane = lax.broadcasted_iota(jnp.int32, angle.shape, 1)
    sine = jnp.sin(angle)
    return jnp.cos(angle), jnp.where(lane < ROPE // 2, -sine, sine)


def column(row, n, shift):
    m = row.shape[1]
    at = lax.broadcasted_iota(jnp.int32, (n, m), 0) + shift
    lane = lax.broadcasted_iota(jnp.int32, (n, m), 1)
    return jnp.sum(jnp.where(at == lane, jnp.broadcast_to(row, (n, m)), 0.0), axis=1, keepdims=True)


def where_am_i():
    z_hi, z_lo = lax.axis_index("zh"), lax.axis_index("zl")
    ctx = ((z_hi * 4 + z_lo) * 4 + lax.axis_index("x")) * 2 + lax.axis_index("yh")
    return lax.axis_index("yl") * 2 + lax.axis_index("core"), ctx * ROWS, z_hi


def key_kernel(own, prev, prev2, gain, bias, pos, freq, out):
    head, first, _ = where_am_i()
    off = pl.multiple_of(head * SUB, SUB)
    own_pos = column(pos[...].astype(jnp.float32), SUB, off)
    tok = (lax.broadcasted_iota(jnp.int32, (SUB, 1), 0) + (first + off)).astype(jnp.float32)
    for slot, ref in enumerate((own, prev, prev2)):
        v = ref[pl.ds(off, SUB), :].astype(jnp.float32)
        c = v - jnp.mean(v, axis=-1, keepdims=True)
        s = jnp.mean(c * c, axis=-1, keepdims=True)
        k = c * lax.rsqrt(s + 1e-06) * gain[...] + bias[...]
        p = own_pos if slot == 0 else tok - float(slot * GROUP)
        cosine, sine = cos_sin(p, freq[...])
        r = turn(k, cosine, sine).astype(jnp.bfloat16)
        for d in range(PEERS):
            out[d, slot] = r


def query_kernel(q, w, pos, freq, out):
    angle = freq[...] * pos[...].astype(jnp.float32)
    cosine, sine = jnp.cos(angle), jnp.sin(angle)
    cosine = jnp.concatenate([cosine, cosine], 1)
    sine = jnp.concatenate([sine, sine], 1)
    wf = w[...].astype(jnp.float32)
    both = jnp.concatenate([wf[: HG // 2], wf[HG // 2 :]], 1)
    half = ROPE // 2
    for p in range(HG // 2):
        x = jnp.concatenate(
            [q[:, h * DH : (h + 1) * DH].astype(jnp.float32) for h in (p, p + HG // 2)], 0
        ).T
        a, b = x[:half], x[half:ROPE]
        x = jnp.concatenate([a * cosine - b * sine, b * cosine + a * sine, x[ROPE:]], 0)
        at = slice(p * DH, (p + 1) * DH)
        out[:DH, at] = x.astype(jnp.bfloat16)
        out[DH:, at] = jnp.broadcast_to(both[p : p + 1], (16, DH)).astype(jnp.bfloat16)


def score_kernel(q0, q1, q2, q3, k, pos, out):
    head, first, group = where_am_i()
    row = lax.broadcasted_iota(jnp.int32, (ROWS, 1), 0) + first
    doc = row - column(pos[...].astype(jnp.float32), ROWS, 0).astype(jnp.int32)

    def one(slot):
        kk = k[:, slot].reshape(NK, DH)
        acc = jnp.zeros((NK, DH), jnp.float32)
        for q in (q0, q1, q2, q3):
            w = q[DH : DH + 1, :].astype(jnp.float32)
            for c in range(0, QT, 512):
                s = jnp.dot(kk, q[:DH, c : c + 512], preferred_element_type=jnp.float32)
                for p in range(0, 512, DH):
                    acc = acc + jnp.maximum(s[:, p : p + DH], 0.0) * w[:, c + p : c + p + DH]
        acc = acc.T
        acc = acc[:ROWS] + acc[ROWS:]
        n = lax.broadcasted_iota(jnp.int32, (1, NK), 1)
        key = (group - slot) * GROUP + (n // DH) * PLANE + ((n % DH) // SUB) * ROWS + head * SUB + n % SUB
        seen = (key >= doc) & (key <= row)
        out[:, slot] = jnp.where(seen, acc * SCALE, 0.0).astype(jnp.bfloat16).reshape(4, SUB, NK)

    live = jnp.where(group == 3, 1, group + 1)
    for slot in range(SLOTS):
        @pl.when(slot < live)
        def _():
            one(slot)

        @pl.when(slot >= live)
        def _():
            out[:, slot] = jnp.zeros((4, SUB, NK), jnp.bfloat16)


def place_kernel(parts, out):
    _, _, group = where_am_i()
    out[...] = jnp.zeros_like(out)
    r = lax.broadcasted_iota(jnp.int32, (DH, PLANE), 0)
    c = lax.broadcasted_iota(jnp.int32, (DH, PLANE), 1)
    base = c - ((r // SUB) * ROWS + r % SUB)
    spread = [jnp.where(base == j * SUB, 1.0, 0.0).astype(jnp.bfloat16) for j in range(4)]
    live = jnp.where(group == 3, 1, group + 1)
    for slot in range(SLOTS):
        @pl.when(slot < live)
        def _():
            full = [jnp.zeros((SUB, PLANE), jnp.float32)] * 4
            for j in range(4):
                x = jnp.concatenate([parts[j, slot, :, z * DH : (z + 1) * DH] for z in range(4)], 0)
                y = jnp.dot(x, spread[j], preferred_element_type=jnp.float32)
                full = [full[z] + y[z * SUB : (z + 1) * SUB] for z in range(4)]
            for z in range(4):
                at = pl.multiple_of((group - slot) * GROUP + z * PLANE, PLANE)
                out[:, pl.ds(at, PLANE)] = full[z]


VMEM = pl.BlockSpec(memory_space=pltpu.VMEM)


def call(kernel, shape, dtype, *args, inside=True):
    if inside:
        out = pltpu.VMEM(shape, dtype)
    else:
        out = jax.ShapeDtypeStruct(shape, dtype)
    return pl.pallas_call(kernel, out_shape=out, in_specs=[VMEM] * len(args), out_specs=VMEM)(*args)


def near(x):
    return pltpu.with_memory_space_constraint(x, pltpu.VMEM)


def program(queries, keys, key_gain, key_bias, head_weights, positions):
    freq = lane_frequencies()
    pos = positions.reshape(1, ROWS)

    prev = lax.ppermute(keys, "zh", [(0, 1), (1, 2)])
    relay = lax.ppermute(keys, "zh", [(0, 3)])
    prev2 = lax.ppermute(relay, "zh", [(3, 2)])

    q0 = call(
        query_kernel, (DH + 16, QT), jnp.bfloat16,
        queries, head_weights.T, pos, jnp.asarray(freq[:, : ROPE // 2].T),
    )
    swap = [(0, 1), (1, 0)]
    q1 = lax.ppermute(q0, "yl", swap)
    q2 = lax.ppermute(q0, "core", swap)
    q3 = lax.ppermute(q1, "core", swap)

    sent = call(
        key_kernel, (PEERS, SLOTS, SUB, DH), jnp.bfloat16,
        keys, near(prev), near(prev2), key_gain.reshape(1, DH), key_bias.reshape(1, DH), pos, jnp.asarray(freq),
    )
    k_all = lax.all_to_all(sent, ("zl", "x", "yh"), 0, 0, tiled=True)

    parts = call(
        score_kernel, (4, SLOTS, SUB, NK), jnp.bfloat16,
        near(q0), near(q1), near(q2), near(q3), near(k_all), pos,
    )
    parts = lax.all_to_all(parts, ("yl", "core"), 0, 0, tiled=True)
    return call(place_kernel, (SUB, 8192), jnp.float32, near(parts), inside=False)


def solution(mesh):
    names = ("zh", "zl", "x", "yh", "yl", "core")
    fine = Mesh(mesh.devices.reshape(4, 4, 4, 2, 2, 2), names)
    ctx, head = names[:4], names[4:]
    in_specs = (P(ctx, head), P(ctx, None), P(), P(), P(ctx, head), P(ctx))
    return jax.shard_map(program, mesh=fine, in_specs=in_specs, out_specs=P(names, None), check_vma=False)
```

```python
import math

import jax
import jax.numpy as jnp
import numpy as np
from jax import lax
from jax.experimental import pallas as pl
from jax.experimental.pallas import tpu as pltpu
from jax.sharding import Mesh
from jax.sharding import PartitionSpec as P

H = 64
DH = 128
ROPE = 64
ROWS = 64
SUB = 16
HG = 16
QT = HG * ROWS
PEERS = 8
SLOTS = 3
NK = PEERS * ROWS
PLANE = 512
GROUP = 4 * PLANE
SCALE = 1.0 / math.sqrt(H * DH)


def yarn_frequencies(rope_dims):
    half_dims = rope_dims // 2
    exponent = np.arange(0, rope_dims, 2) / rope_dims
    extra_freq = 1.0 / 10000.0**exponent
    inter_freq = extra_freq / 40.0

    def correction(beta):
        return rope_dims * math.log(4096.0 / (beta * 2.0 * math.pi)) / (2.0 * math.log(10000.0))

    low_dim = max(math.floor(correction(32.0)), 0)
    high_dim = min(math.ceil(correction(1.0)), rope_dims - 1)
    ramp_values = np.clip((np.arange(half_dims) - low_dim) / (high_dim - low_dim), 0.0, 1.0)
    return (inter_freq * ramp_values + extra_freq * (1.0 - ramp_values)).astype(np.float32)


def lane_frequencies():
    f = yarn_frequencies(ROPE)
    return np.concatenate([f, f, np.zeros(DH - ROPE, np.float32)])[None, :]


def turn(x, cosine, sine):
    lane = lax.broadcasted_iota(jnp.int32, x.shape, 1)
    half = ROPE // 2
    other = jnp.where(lane < half, pltpu.roll(x, DH - half, 1), pltpu.roll(x, half, 1))
    return x * cosine + other * sine


def cos_sin(pos, freq):
    angle = pos * freq
    lane = lax.broadcasted_iota(jnp.int32, angle.shape, 1)
    sine = jnp.sin(angle)
    return jnp.cos(angle), jnp.where(lane < ROPE // 2, -sine, sine)


def column(row, n, shift):
    m = row.shape[1]
    at = lax.broadcasted_iota(jnp.int32, (n, m), 0) + shift
    lane = lax.broadcasted_iota(jnp.int32, (n, m), 1)
    return jnp.sum(jnp.where(at == lane, jnp.broadcast_to(row, (n, m)), 0.0), axis=1, keepdims=True)


def where_am_i():
    z_hi, z_lo = lax.axis_index("zh"), lax.axis_index("zl")
    ctx = ((z_hi * 4 + z_lo) * 4 + lax.axis_index("x")) * 2 + lax.axis_index("yh")
    head = lax.axis_index("yl") * 2 + lax.axis_index("core")
    return head, ctx * ROWS, z_hi, z_lo ^ head ^ (2 * lax.axis_index("yh"))


def prepare_kernel(keys, gain, bias, q, w, pos, freq, freq_col, out_k, out_q):
    v = keys[...].astype(jnp.float32)
    c = v - jnp.mean(v, axis=-1, keepdims=True)
    s = jnp.mean(c * c, axis=-1, keepdims=True)
    k = c * lax.rsqrt(s + 1e-06) * gain[...] + bias[...]
    cosine, sine = cos_sin(column(pos[...].astype(jnp.float32), ROWS, 0), freq[...])
    out_k[...] = turn(k, cosine, sine).astype(jnp.bfloat16)
    query_kernel(q, w, pos, freq_col, out_q)


def pack_kernel(mine, own, prev_1, prev_2, prev2, out):
    _, _, group, z = where_am_i()
    first = jnp.where(z == lax.axis_index("zl"), mine[...], own[...])
    prev = jnp.where(group == 1, prev_1[...], prev_2[...])
    for slot, x in enumerate((first, prev, prev2[...])):
        for d in range(PEERS):
            out[d, slot] = x


def query_kernel(q, w, pos, freq, out):
    angle = freq[...] * pos[...].astype(jnp.float32)
    cosine, sine = jnp.cos(angle), jnp.sin(angle)
    cosine = jnp.concatenate([cosine, cosine], 1)
    sine = jnp.concatenate([sine, sine], 1)
    wf = w[...].astype(jnp.float32)
    both = jnp.concatenate([wf[: HG // 2], wf[HG // 2 :]], 1)
    half = ROPE // 2
    for p in range(HG // 2):
        x = jnp.concatenate(
            [q[:, h * DH : (h + 1) * DH].astype(jnp.float32) for h in (p, p + HG // 2)], 0
        ).T
        a, b = x[:half], x[half:ROPE]
        x = jnp.concatenate([a * cosine - b * sine, b * cosine + a * sine, x[ROPE:]], 0)
        at = slice(p * DH, (p + 1) * DH)
        out[:DH, at] = x.astype(jnp.bfloat16)
        out[DH:, at] = jnp.broadcast_to(both[p : p + 1], (16, DH)).astype(jnp.bfloat16)


def score_kernel(q0, q1, q2, q3, k, pos, out):
    _, first, group, z = where_am_i()
    row = lax.broadcasted_iota(jnp.int32, (ROWS, 1), 0) + first
    doc = row - column(pos[...].astype(jnp.float32), ROWS, 0).astype(jnp.int32)

    def one(slot):
        kk = k[:, slot].reshape(NK, DH)
        acc = jnp.zeros((NK, DH), jnp.float32)
        for q in (q0, q1, q2, q3):
            w = q[DH : DH + 1, :].astype(jnp.float32)
            for c in range(0, QT, 512):
                s = jnp.dot(kk, q[:DH, c : c + 512], preferred_element_type=jnp.float32)
                for p in range(0, 512, DH):
                    acc = acc + jnp.maximum(s[:, p : p + DH], 0.0) * w[:, c + p : c + p + DH]
        acc = acc.T
        acc = acc[:ROWS] + acc[ROWS:]
        n = lax.broadcasted_iota(jnp.int32, (1, NK), 1)
        key = (group - slot) * GROUP + z * PLANE + n
        seen = (key >= doc) & (key <= row)
        out[:, slot] = jnp.where(seen, acc * SCALE, 0.0).astype(jnp.bfloat16).reshape(4, SUB, NK)

    live = jnp.where(group == 3, 1, group + 1)
    for slot in range(SLOTS):
        @pl.when(slot < live)
        def _():
            one(slot)

        @pl.when(slot >= live)
        def _():
            out[:, slot] = jnp.zeros((4, SUB, NK), jnp.bfloat16)


def place_kernel(parts, out):
    head, _, group, z = where_am_i()
    out[...] = jnp.zeros_like(out)
    live = jnp.where(group == 3, 1, group + 1)
    for slot in range(SLOTS):
        @pl.when(slot < live)
        def _():
            for j in range(4):
                at = pl.multiple_of((group - slot) * GROUP + (z ^ head ^ j) * PLANE, PLANE)
                out[:, pl.ds(at, PLANE)] = parts[j, slot].astype(jnp.float32)


VMEM = pl.BlockSpec(memory_space=pltpu.VMEM)


def call(kernel, shape, dtype, *args, inside=True):
    if inside:
        out = pltpu.VMEM(shape, dtype)
    else:
        out = jax.ShapeDtypeStruct(shape, dtype)
    return pl.pallas_call(kernel, out_shape=out, in_specs=[VMEM] * len(args), out_specs=VMEM)(*args)


def near(x):
    return pltpu.with_memory_space_constraint(x, pltpu.VMEM)


LINE = ("zh", "zl", "yh", "yl", "core")


def hop(src, dst, cross):
    def at(g, z, j):
        return (g * 4 + z) * 8 + j

    return [
        (at(src, z, j), at(dst, z ^ m if cross else z, j))
        for z in range(4) for j in range(8) for m in ((j & 3) ^ (j >> 2) * 2,) if src != dst or m
    ]


NEAR = [[(x * 2 + h) * 2 + (t ^ h) for x in range(4) for h in range(2)] for t in range(2)]


def program(queries, keys, key_gain, key_bias, head_weights, positions):
    freq = lane_frequencies()
    pos = positions.reshape(1, ROWS)

    mine, q0 = pl.pallas_call(
        prepare_kernel,
        out_shape=(pltpu.VMEM((ROWS, DH), jnp.bfloat16), pltpu.VMEM((DH + 16, QT), jnp.bfloat16)),
        in_specs=[VMEM] * 8, out_specs=(VMEM, VMEM), name="prepare",
    )(
        keys, key_gain.reshape(1, DH), key_bias.reshape(1, DH), queries, head_weights.T, pos,
        jnp.asarray(freq), jnp.asarray(freq[:, : ROPE // 2].T),
    )
    prev_1 = lax.ppermute(mine, LINE, hop(0, 1, True))
    prev_2 = lax.ppermute(mine, LINE, hop(1, 2, True))
    own = lax.ppermute(mine, LINE, sum((hop(g, g, True) for g in range(4)), []))
    prev2 = lax.ppermute(prev_1, LINE, hop(1, 2, False))

    swap = [(0, 1), (1, 0)]
    q1 = lax.ppermute(q0, "yl", swap)
    q2 = lax.ppermute(q0, "core", swap)
    q3 = lax.ppermute(q1, "core", swap)

    sent = call(
        pack_kernel, (PEERS, SLOTS, ROWS, DH), jnp.bfloat16,
        near(mine), near(own), near(prev_1), near(prev_2), near(prev2),
    )
    k_all = lax.all_to_all(
        sent, ("x", "yh", "yl"), 0, 0, axis_index_groups=NEAR, tiled=True
    )

    parts = call(
        score_kernel, (4, SLOTS, SUB, NK), jnp.bfloat16,
        near(q0), near(q1), near(q2), near(q3), near(k_all), near(pos),
    )
    parts = lax.all_to_all(parts, ("yl", "core"), 0, 0, tiled=True)
    return call(place_kernel, (SUB, 8192), jnp.float32, near(parts), inside=False)


def solution(mesh):
    names = ("zh", "zl", "x", "yh", "yl", "core")
    fine = Mesh(mesh.devices.reshape(4, 4, 4, 2, 2, 2), names)
    ctx, head = names[:4], names[4:]
    in_specs = (P(ctx, head), P(ctx, None), P(), P(), P(ctx, head), P(ctx))
    return jax.shard_map(program, mesh=fine, in_specs=in_specs, out_specs=P(names, None), check_vma=False)
```

```python
import math

import jax
import jax.numpy as jnp
import numpy as np
from jax import lax
from jax.experimental import pallas as pl
from jax.experimental.pallas import tpu as pltpu
from jax.sharding import Mesh
from jax.sharding import PartitionSpec as P

H = 64
DH = 128
ROPE = 64
ROWS = 64
SUB = 16
HG = 16
QT = HG * ROWS
PEERS = 8
SLOTS = 3
NK = PEERS * ROWS
PLANE = 512
GROUP = 4 * PLANE
LAST_EARLY = 6
SCALE = 1.0 / math.sqrt(H * DH)


def yarn_frequencies(rope_dims):
    half_dims = rope_dims // 2
    exponent = np.arange(0, rope_dims, 2) / rope_dims
    extra_freq = 1.0 / 10000.0**exponent
    inter_freq = extra_freq / 40.0

    def correction(beta):
        return rope_dims * math.log(4096.0 / (beta * 2.0 * math.pi)) / (2.0 * math.log(10000.0))

    low_dim = max(math.floor(correction(32.0)), 0)
    high_dim = min(math.ceil(correction(1.0)), rope_dims - 1)
    ramp_values = np.clip((np.arange(half_dims) - low_dim) / (high_dim - low_dim), 0.0, 1.0)
    return (inter_freq * ramp_values + extra_freq * (1.0 - ramp_values)).astype(np.float32)


def turned(raw, gain, bias, cosine, sine):
    v = raw.astype(jnp.float32)
    c = v - jnp.mean(v, axis=-1, keepdims=True)
    s = jnp.mean(c * c, axis=-1, keepdims=True)
    k = c * lax.rsqrt(s + 1e-06) * gain + bias
    return rotated(jnp.concatenate([k, k], 0).T, cosine, sine).T[:ROWS].astype(jnp.bfloat16)


def rotated(x, cosine, sine):
    half = ROPE // 2
    cosine = jnp.concatenate([cosine, cosine], 1)
    sine = jnp.concatenate([sine, sine], 1)
    a, b = x[:half], x[half:ROPE]
    return jnp.concatenate([a * cosine - b * sine, b * cosine + a * sine, x[ROPE:]], 0)


def column(row, n, shift):
    m = row.shape[1]
    at = lax.broadcasted_iota(jnp.int32, (n, m), 0) + shift
    lane = lax.broadcasted_iota(jnp.int32, (n, m), 1)
    return jnp.sum(jnp.where(at == lane, jnp.broadcast_to(row, (n, m)), 0.0), axis=1, keepdims=True)


def where_am_i():
    z_hi, z_lo = lax.axis_index("zh"), lax.axis_index("zl")
    ctx = ((z_hi * 4 + z_lo) * 4 + lax.axis_index("x")) * 2 + lax.axis_index("yh")
    head = lax.axis_index("yl") * 2 + lax.axis_index("core")
    return head, ctx * ROWS, z_hi, z_lo ^ head ^ (2 * lax.axis_index("yh"))


def turn_queries(q, w, cosine, sine, out):
    wf = w[...].astype(jnp.float32)
    both = jnp.concatenate([wf[: HG // 2], wf[HG // 2 :]], 1)
    for p in range(HG // 2):
        x = jnp.concatenate(
            [q[:, h * DH : (h + 1) * DH].astype(jnp.float32) for h in (p, p + HG // 2)], 0
        ).T
        at = slice(p * DH, (p + 1) * DH)
        out[:DH, at] = rotated(x, cosine, sine).astype(jnp.bfloat16)
        out[DH:, at] = jnp.broadcast_to(both[p : p + 1], (16, DH)).astype(jnp.bfloat16)


def is_early():
    return lax.axis_index("zh") * 4 + lax.axis_index("zl") <= LAST_EARLY


def sends_on():
    return lax.axis_index("zh") < 2


def fetch(pairs, sems):
    copies = [pltpu.make_async_copy(src, dst, sems.at[i]) for i, (src, dst) in enumerate(pairs)]
    for c in copies:
        c.start()
    for c in copies:
        c.wait()


def early_kernel(*refs):
    far, out_k, out_q, held, sems = refs[:7], refs[7], refs[8], refs[9:16], refs[16]

    @pl.when(is_early())
    def _():
        fetch(zip(far, held), sems)
        keys, gain, bias, pos, freq, w, q = held
        angle = freq[...] * pos[...].astype(jnp.float32)
        cosine, sine = jnp.cos(angle), jnp.sin(angle)
        out_k[...] = turned(keys[...], gain[...], bias[...], cosine, sine)
        turn_queries(q, w, cosine, sine, out_q)


def late_keys_kernel(*refs):
    far, before, out_q, out_k, held, sems = refs[:7], refs[8], refs[9], refs[10], refs[11:18], refs[18]
    keys, gain, bias, pos, freq, w, q = held
    late = jnp.logical_not(is_early())

    @pl.when(is_early())
    def _():
        out_k[...] = before[...]

    @pl.when(late & sends_on())
    def _():
        fetch(zip(far, held), sems)
        angle = freq[...] * pos[...].astype(jnp.float32)
        cosine, sine = jnp.cos(angle), jnp.sin(angle)
        out_k[...] = turned(keys[...], gain[...], bias[...], cosine, sine)
        turn_queries(q, w, cosine, sine, out_q)

    @pl.when(late & jnp.logical_not(sends_on()))
    def _():
        fetch(tuple(zip(far, held))[:5], sems)
        angle = freq[...] * pos[...].astype(jnp.float32)
        out_k[...] = turned(keys[...], gain[...], bias[...], jnp.cos(angle), jnp.sin(angle))


def late_queries_kernel(*refs):
    far, out_q, held, sems = refs[:4], refs[5], refs[6:10], refs[10]

    @pl.when(jnp.logical_not(is_early() | sends_on()))
    def _():
        fetch(zip(far, held), sems)
        pos, freq, w, q = held
        angle = freq[...] * pos[...].astype(jnp.float32)
        turn_queries(q, w, jnp.cos(angle), jnp.sin(angle), out_q)


def prepare(kernel, sources, shapes, before=(), kept=0):
    n = len(sources)
    return pl.pallas_call(
        kernel,
        out_shape=tuple(pltpu.VMEM(shape, jnp.bfloat16) for shape in shapes),
        in_specs=[ANY] * n + [VMEM] * len(before),
        out_specs=(VMEM,) * len(shapes),
        input_output_aliases={n + i: i for i in range(kept)},
        scratch_shapes=[pltpu.VMEM(x.shape, x.dtype) for x in sources] + [pltpu.SemaphoreType.DMA((n,))],
    )(*sources, *[near(x) for x in before])


def pack_kernel(mine, own, prev_1, prev_2, prev2, out):
    _, _, group, z = where_am_i()
    first = jnp.where(z == lax.axis_index("zl"), mine[...], own[...])
    prev = jnp.where(group == 1, prev_1[...], prev_2[...])
    for slot, x in enumerate((first, prev, prev2[...])):
        for d in range(PEERS):
            out[d, slot] = x


def score_kernel(q0, q1, q2, q3, k, pos, out):
    _, first, group, z = where_am_i()
    row = lax.broadcasted_iota(jnp.int32, (ROWS, 1), 0) + first
    doc = row - column(pos[...].astype(jnp.float32), ROWS, 0).astype(jnp.int32)

    def one(slot, start, n):
        peers = slice(start // ROWS, (start + n) // ROWS)
        kk = k[peers, slot].reshape(n, DH)
        acc = jnp.zeros((n, DH), jnp.float32)
        for q in (q0, q1, q2, q3):
            w = q[DH : DH + 1, :].astype(jnp.float32)
            for c in range(0, QT, 512):
                s = jnp.dot(kk, q[:DH, c : c + 512], preferred_element_type=jnp.float32)
                for p in range(0, 512, DH):
                    acc = acc + jnp.maximum(s[:, p : p + DH], 0.0) * w[:, c + p : c + p + DH]
        acc = acc.T
        acc = acc[:ROWS] + acc[ROWS:]
        key = plane_start(slot) + start + lax.broadcasted_iota(jnp.int32, (1, n), 1)
        seen = (key >= doc) & (key <= row)
        out[:, slot, :, start : start + n] = (
            jnp.where(seen, acc * SCALE, 0.0).astype(jnp.bfloat16).reshape(4, SUB, n)
        )

    def plane_start(slot):
        return (group - slot) * GROUP + z * PLANE

    for start, n in ((0, 128), (128, 128), (256, 256)):
        reached = plane_start(0) + start < first + ROWS

        @pl.when(reached)
        def _():
            one(0, start, n)

        @pl.when(jnp.logical_not(reached))
        def _():
            out[:, 0, :, start : start + n] = jnp.zeros((4, SUB, n), jnp.bfloat16)

    for slot in range(1, SLOTS):
        live = (slot <= group) & (group < 3)

        @pl.when(live)
        def _():
            one(slot, 0, NK)

        @pl.when(jnp.logical_not(live))
        def _():
            out[:, slot] = jnp.zeros((4, SUB, NK), jnp.bfloat16)


def place_kernel(parts, out):
    head, _, group, z = where_am_i()
    out[...] = jnp.zeros_like(out)
    live = jnp.where(group == 3, 1, group + 1)
    for slot in range(SLOTS):
        @pl.when(slot < live)
        def _():
            for j in range(4):
                at = pl.multiple_of((group - slot) * GROUP + (z ^ head ^ j) * PLANE, PLANE)
                out[:, pl.ds(at, PLANE)] = parts[j, slot].astype(jnp.float32)


VMEM = pl.BlockSpec(memory_space=pltpu.VMEM)
ANY = pl.BlockSpec(memory_space=pl.ANY)


def call(kernel, shape, dtype, *args, inside=True):
    if inside:
        out = pltpu.VMEM(shape, dtype)
    else:
        out = jax.ShapeDtypeStruct(shape, dtype)
    return pl.pallas_call(kernel, out_shape=out, in_specs=[VMEM] * len(args), out_specs=VMEM)(*args)


def near(x):
    return pltpu.with_memory_space_constraint(x, pltpu.VMEM)


LINE = ("zh", "zl", "yh", "yl", "core")


def hop(src, dst, cross):
    def at(g, z, j):
        return (g * 4 + z) * 8 + j

    return [
        (at(src, z, j), at(dst, z ^ m if cross else z, j))
        for z in range(4) for j in range(8) for m in ((j & 3) ^ (j >> 2) * 2,) if src != dst or m
    ]


NEAR = [[(x * 2 + h) * 2 + (t ^ h) for x in range(4) for h in range(2)] for t in range(2)]


def program(queries, keys, key_gain, key_bias, head_weights, positions):
    freq = jnp.asarray(yarn_frequencies(ROPE)[:, None])
    gain, bias = key_gain.reshape(1, DH), key_bias.reshape(1, DH)
    pos = positions.reshape(1, ROWS)
    weights = head_weights.T

    key_shape, query_shape = (ROWS, DH), (DH + 16, QT)

    mine, q_early = prepare(early_kernel, (keys, gain, bias, pos, freq, weights, queries), (key_shape, query_shape))
    prev_1 = lax.ppermute(mine, LINE, hop(0, 1, True))
    q_early, mine = prepare(
        late_keys_kernel, (keys, gain, bias, pos, freq, weights, queries),
        (query_shape, key_shape), (q_early, mine), 1,
    )
    prev_2 = lax.ppermute(mine, LINE, hop(1, 2, True))
    own = lax.ppermute(mine, LINE, sum((hop(g, g, True) for g in range(4)), []))
    prev2 = lax.ppermute(prev_1, LINE, hop(1, 2, False))
    (q0,) = prepare(late_queries_kernel, (pos, freq, weights, queries), (query_shape,), (q_early,), 1)
    swap = [(0, 1), (1, 0)]
    q1 = lax.ppermute(q0, "yl", swap)
    q2 = lax.ppermute(q0, "core", swap)
    q3 = lax.ppermute(q1, "core", swap)

    sent = call(
        pack_kernel, (PEERS, SLOTS, ROWS, DH), jnp.bfloat16,
        near(mine), near(own), near(prev_1), near(prev_2), near(prev2),
    )
    k_all = lax.all_to_all(
        sent, ("x", "yh", "yl"), 0, 0, axis_index_groups=NEAR, tiled=True
    )

    parts = call(
        score_kernel, (4, SLOTS, SUB, NK), jnp.bfloat16,
        near(q0), near(q1), near(q2), near(q3), near(k_all), near(pos),
    )
    parts = lax.all_to_all(parts, ("yl", "core"), 0, 0, tiled=True)
    return call(place_kernel, (SUB, 8192), jnp.float32, near(parts), inside=False)


def solution(mesh):
    names = ("zh", "zl", "x", "yh", "yl", "core")
    fine = Mesh(mesh.devices.reshape(4, 4, 4, 2, 2, 2), names)
    ctx, head = names[:4], names[4:]
    in_specs = (P(ctx, head), P(ctx, None), P(), P(), P(ctx, head), P(ctx))
    return jax.shard_map(program, mesh=fine, in_specs=in_specs, out_specs=P(names, None), check_vma=False)
```

```python
import functools
import math

import jax
import jax.numpy as jnp
import numpy as np
from jax import lax
from jax.experimental import pallas as pl
from jax.experimental.pallas import tpu as pltpu
from jax.sharding import Mesh
from jax.sharding import PartitionSpec as P

H = 64
DH = 128
ROPE = 64
ROWS = 64
SUB = 16
HG = 16
QT = HG * ROWS
PEERS = 8
SLOTS = 3
NK = PEERS * ROWS
PLANE = 512
GROUP = 4 * PLANE
LAST_EARLY = 3
SCALE = 1.0 / math.sqrt(H * DH)


def yarn_frequencies(rope_dims):
    half_dims = rope_dims // 2
    exponent = np.arange(0, rope_dims, 2) / rope_dims
    extra_freq = 1.0 / 10000.0**exponent
    inter_freq = extra_freq / 40.0

    def correction(beta):
        return rope_dims * math.log(4096.0 / (beta * 2.0 * math.pi)) / (2.0 * math.log(10000.0))

    low_dim = max(math.floor(correction(32.0)), 0)
    high_dim = min(math.ceil(correction(1.0)), rope_dims - 1)
    ramp_values = np.clip((np.arange(half_dims) - low_dim) / (high_dim - low_dim), 0.0, 1.0)
    return (inter_freq * ramp_values + extra_freq * (1.0 - ramp_values)).astype(np.float32)


def turned(raw, gain, bias, cosine, sine):
    v = raw.astype(jnp.float32)
    c = v - jnp.mean(v, axis=-1, keepdims=True)
    s = jnp.mean(c * c, axis=-1, keepdims=True)
    k = c * lax.rsqrt(s + 1e-06) * gain + bias
    return rotated(jnp.concatenate([k, k], 0).T, cosine, sine).T[:ROWS].astype(jnp.bfloat16)


def rotated(x, cosine, sine):
    half = ROPE // 2
    cosine = jnp.concatenate([cosine, cosine], 1)
    sine = jnp.concatenate([sine, sine], 1)
    a, b = x[:half], x[half:ROPE]
    return jnp.concatenate([a * cosine - b * sine, b * cosine + a * sine, x[ROPE:]], 0)


def column(row, n, shift):
    m = row.shape[1]
    at = lax.broadcasted_iota(jnp.int32, (n, m), 0) + shift
    lane = lax.broadcasted_iota(jnp.int32, (n, m), 1)
    return jnp.sum(jnp.where(at == lane, jnp.broadcast_to(row, (n, m)), 0.0), axis=1, keepdims=True)


def where_am_i():
    z_hi, z_lo = lax.axis_index("zh"), lax.axis_index("zl")
    ctx = ((z_hi * 4 + z_lo) * 4 + lax.axis_index("x")) * 2 + lax.axis_index("yh")
    head = lax.axis_index("yl") * 2 + lax.axis_index("core")
    return head, ctx * ROWS, z_hi, z_lo ^ head ^ (2 * lax.axis_index("yh"))


def turn_queries(q, w, cosine, sine, out):
    wf = w[...].astype(jnp.float32)
    both = jnp.concatenate([wf[: HG // 2], wf[HG // 2 :]], 1)
    for p in range(HG // 2):
        x = jnp.concatenate(
            [q[:, h * DH : (h + 1) * DH].astype(jnp.float32) for h in (p, p + HG // 2)], 0
        ).T
        at = slice(p * DH, (p + 1) * DH)
        out[:DH, at] = rotated(x, cosine, sine).astype(jnp.bfloat16)
        out[DH:, at] = jnp.broadcast_to(both[p : p + 1], (16, DH)).astype(jnp.bfloat16)


def turn(k):
    plane = lax.axis_index("zh") * 4 + lax.axis_index("zl")
    group_2 = lax.axis_index("zh") == 2
    return (plane <= LAST_EARLY, (plane > LAST_EARLY) & jnp.logical_not(group_2), group_2)[k]


def fetch(pairs, sems):
    copies = [pltpu.make_async_copy(src, dst, sems.at[i]) for i, (src, dst) in enumerate(pairs)]
    for c in copies:
        c.start()
    for c in copies:
        c.wait()


def prepare_kernel(k, *refs):
    n = 7
    far, refs = refs[:n], refs[n:]
    if k:
        before, refs = refs[0], refs[2:]
    out_q, out_k, held, sems = refs[0], refs[1], refs[2 : 2 + n], refs[2 + n]

    if k:
        @pl.when(jnp.logical_not(turn(k)))
        def _():
            out_k[...] = before[...]

    @pl.when(turn(k))
    def _():
        fetch(zip(far, held), sems)
        keys, gain, bias, pos, freq, w, q = held
        angle = freq[...] * pos[...].astype(jnp.float32)
        cosine, sine = jnp.cos(angle), jnp.sin(angle)
        out_k[...] = turned(keys[...], gain[...], bias[...], cosine, sine)
        turn_queries(q, w, cosine, sine, out_q)


def prepare(k, sources, before=()):
    n = len(sources)
    return pl.pallas_call(
        functools.partial(prepare_kernel, k),
        out_shape=(pltpu.VMEM((DH + 16, QT), jnp.bfloat16), pltpu.VMEM((ROWS, DH), jnp.bfloat16)),
        in_specs=[ANY] * n + [VMEM] * len(before),
        out_specs=(VMEM, VMEM),
        input_output_aliases={n + 1: 0} if k else {},
        scratch_shapes=[pltpu.VMEM(x.shape, x.dtype) for x in sources] + [pltpu.SemaphoreType.DMA((n,))],
    )(*sources, *[near(x) for x in before])


def pack_kernel(own_0, own_13, own_2, from_0, near_by, far_off, out):
    group = lax.axis_index("zh")
    own = jnp.where(group == 0, own_0[...], jnp.where(group == 2, own_2[...], own_13[...]))
    last = jnp.where(group == 1, from_0[...], near_by[...])
    for slot, x in enumerate((own, last, far_off[...])):
        for d in range(PEERS):
            out[d, slot] = x


def score_kernel(q0, q1, q2, q3, k, pos, out):
    _, first, group, z = where_am_i()
    row = lax.broadcasted_iota(jnp.int32, (ROWS, 1), 0) + first
    doc = row - column(pos[...].astype(jnp.float32), ROWS, 0).astype(jnp.int32)

    def one(slot, start, n):
        peers = slice(start // ROWS, (start + n) // ROWS)
        kk = k[peers, slot].reshape(n, DH)
        acc = jnp.zeros((n, DH), jnp.float32)
        for q in (q0, q1, q2, q3):
            w = q[DH : DH + 1, :].astype(jnp.float32)
            for c in range(0, QT, 512):
                s = jnp.dot(kk, q[:DH, c : c + 512], preferred_element_type=jnp.float32)
                for p in range(0, 512, DH):
                    acc = acc + jnp.maximum(s[:, p : p + DH], 0.0) * w[:, c + p : c + p + DH]
        acc = acc.T
        acc = acc[:ROWS] + acc[ROWS:]
        key = plane_start(slot) + start + lax.broadcasted_iota(jnp.int32, (1, n), 1)
        seen = (key >= doc) & (key <= row)
        out[:, slot, :, start : start + n] = (
            jnp.where(seen, acc * SCALE, 0.0).astype(jnp.bfloat16).reshape(4, SUB, n)
        )

    def plane_start(slot):
        return (group - slot) * GROUP + z * PLANE

    for start, n in ((0, 128), (128, 128), (256, 256)):
        reached = plane_start(0) + start < first + ROWS

        @pl.when(reached)
        def _():
            one(0, start, n)

        @pl.when(jnp.logical_not(reached))
        def _():
            out[:, 0, :, start : start + n] = jnp.zeros((4, SUB, n), jnp.bfloat16)

    for slot in range(1, SLOTS):
        live = (slot <= group) & (group < 3)

        @pl.when(live)
        def _():
            one(slot, 0, NK)

        @pl.when(jnp.logical_not(live))
        def _():
            out[:, slot] = jnp.zeros((4, SUB, NK), jnp.bfloat16)


def place_kernel(parts, out):
    head, _, group, z = where_am_i()
    out[...] = jnp.zeros_like(out)
    live = jnp.where(group == 3, 1, group + 1)
    for slot in range(SLOTS):
        @pl.when(slot < live)
        def _():
            for j in range(4):
                at = pl.multiple_of((group - slot) * GROUP + (z ^ head ^ j) * PLANE, PLANE)
                out[:, pl.ds(at, PLANE)] = parts[j, slot].astype(jnp.float32)


VMEM = pl.BlockSpec(memory_space=pltpu.VMEM)
ANY = pl.BlockSpec(memory_space=pl.ANY)


def call(kernel, shape, dtype, *args, inside=True):
    if inside:
        out = pltpu.VMEM(shape, dtype)
    else:
        out = jax.ShapeDtypeStruct(shape, dtype)
    return pl.pallas_call(kernel, out_shape=out, in_specs=[VMEM] * len(args), out_specs=VMEM)(*args)


def near(x):
    return pltpu.with_memory_space_constraint(x, pltpu.VMEM)


LINE = ("zh", "zl", "yh", "yl", "core")


def hop(src, dst, cross):
    def at(g, z, j):
        return (g * 4 + z) * 8 + j

    return [
        (at(src, z, j), at(dst, z ^ m if cross else z, j))
        for z in range(4) for j in range(8) for m in ((j & 3) ^ (j >> 2) * 2,)
    ]


NEAR = [[(x * 2 + h) * 2 + (t ^ h) for x in range(4) for h in range(2)] for t in range(2)]


def program(queries, keys, key_gain, key_bias, head_weights, positions):
    freq = jnp.asarray(yarn_frequencies(ROPE)[:, None])
    gain, bias = key_gain.reshape(1, DH), key_bias.reshape(1, DH)
    pos = positions.reshape(1, ROWS)
    weights = head_weights.T

    sources = (keys, gain, bias, pos, freq, weights, queries)

    q, mine = prepare(0, sources)
    own_0 = lax.ppermute(mine, LINE, hop(0, 0, True))
    from_0 = lax.ppermute(own_0, LINE, hop(0, 1, False))
    q, mine = prepare(1, sources, (mine, q))
    own_13 = lax.ppermute(mine, LINE, hop(1, 1, True) + hop(3, 3, True))
    far_off = lax.ppermute(from_0, LINE, hop(1, 2, False))
    q0, mine = prepare(2, sources, (mine, q))
    swap = [(0, 1), (1, 0)]
    q1 = lax.ppermute(q0, "yl", swap)
    near_by = lax.ppermute(own_13, LINE, hop(1, 2, False))
    own_2 = lax.ppermute(mine, LINE, hop(2, 2, True))
    q2 = lax.ppermute(q0, "core", swap)
    q3 = lax.ppermute(q1, "core", swap)

    sent = call(
        pack_kernel, (PEERS, SLOTS, ROWS, DH), jnp.bfloat16,
        near(own_0), near(own_13), near(own_2), near(from_0), near(near_by), near(far_off),
    )
    k_all = lax.all_to_all(
        sent, ("x", "yh", "yl"), 0, 0, axis_index_groups=NEAR, tiled=True
    )

    parts = call(
        score_kernel, (4, SLOTS, SUB, NK), jnp.bfloat16,
        near(q0), near(q1), near(q2), near(q3), near(k_all), near(pos),
    )
    parts = lax.all_to_all(parts, ("yl", "core"), 0, 0, tiled=True)
    return call(place_kernel, (SUB, 8192), jnp.float32, near(parts), inside=False)


def solution(mesh):
    names = ("zh", "zl", "x", "yh", "yl", "core")
    fine = Mesh(mesh.devices.reshape(4, 4, 4, 2, 2, 2), names)
    ctx, head = names[:4], names[4:]
    in_specs = (P(ctx, head), P(ctx, None), P(), P(), P(ctx, head), P(ctx))
    return jax.shard_map(program, mesh=fine, in_specs=in_specs, out_specs=P(names, None), check_vma=False)
```

```python
import functools
import math

import jax
import jax.numpy as jnp
import numpy as np
from jax import lax
from jax.experimental import pallas as pl
from jax.experimental.pallas import tpu as pltpu
from jax.sharding import Mesh
from jax.sharding import PartitionSpec as P

H = 64
DH = 128
ROPE = 64
ROWS = 64
SUB = 16
HG = 16
QT = HG * ROWS
PEERS = 8
SLOTS = 3
NK = PEERS * ROWS
PLANE = 512
GROUP = 4 * PLANE
LAST_EARLY = 3
SCALE = 1.0 / math.sqrt(H * DH)


def yarn_frequencies(rope_dims):
    half_dims = rope_dims // 2
    exponent = np.arange(0, rope_dims, 2) / rope_dims
    extra_freq = 1.0 / 10000.0**exponent
    inter_freq = extra_freq / 40.0

    def correction(beta):
        return rope_dims * math.log(4096.0 / (beta * 2.0 * math.pi)) / (2.0 * math.log(10000.0))

    low_dim = max(math.floor(correction(32.0)), 0)
    high_dim = min(math.ceil(correction(1.0)), rope_dims - 1)
    ramp_values = np.clip((np.arange(half_dims) - low_dim) / (high_dim - low_dim), 0.0, 1.0)
    return (inter_freq * ramp_values + extra_freq * (1.0 - ramp_values)).astype(np.float32)


def turned(raw, gain, bias, cosine, sine):
    v = raw.astype(jnp.float32)
    c = v - jnp.mean(v, axis=-1, keepdims=True)
    s = jnp.mean(c * c, axis=-1, keepdims=True)
    k = c * lax.rsqrt(s + 1e-06) * gain + bias
    return rotated(jnp.concatenate([k, k], 0).T, cosine, sine).T[:ROWS].astype(jnp.bfloat16)


def rotated(x, cosine, sine):
    half = ROPE // 2
    cosine = jnp.concatenate([cosine, cosine], 1)
    sine = jnp.concatenate([sine, sine], 1)
    a, b = x[:half], x[half:ROPE]
    return jnp.concatenate([a * cosine - b * sine, b * cosine + a * sine, x[ROPE:]], 0)


def column(row, n, shift):
    m = row.shape[1]
    at = lax.broadcasted_iota(jnp.int32, (n, m), 0) + shift
    lane = lax.broadcasted_iota(jnp.int32, (n, m), 1)
    return jnp.sum(jnp.where(at == lane, jnp.broadcast_to(row, (n, m)), 0.0), axis=1, keepdims=True)


def where_am_i():
    z_hi, z_lo = lax.axis_index("zh"), lax.axis_index("zl")
    ctx = ((z_hi * 4 + z_lo) * 4 + lax.axis_index("x")) * 2 + lax.axis_index("yh")
    head = lax.axis_index("yl") * 2 + lax.axis_index("core")
    return head, ctx * ROWS, z_hi, z_lo ^ head ^ (2 * lax.axis_index("yh"))


def turn_queries(q, w, cosine, sine, out):
    wf = w[...].astype(jnp.float32)
    both = jnp.concatenate([wf[: HG // 2], wf[HG // 2 :]], 1)
    for p in range(HG // 2):
        x = jnp.concatenate(
            [q[:, h * DH : (h + 1) * DH].astype(jnp.float32) for h in (p, p + HG // 2)], 0
        ).T
        at = slice(p * DH, (p + 1) * DH)
        out[:DH, at] = rotated(x, cosine, sine).astype(jnp.bfloat16)
        out[DH:, at] = jnp.broadcast_to(both[p : p + 1], (16, DH)).astype(jnp.bfloat16)


def turn(k):
    plane = lax.axis_index("zh") * 4 + lax.axis_index("zl")
    group_2 = lax.axis_index("zh") == 2
    return (plane <= LAST_EARLY, (plane > LAST_EARLY) & jnp.logical_not(group_2), group_2)[k]


def fetch(pairs, sems):
    copies = [pltpu.make_async_copy(src, dst, sems.at[i]) for i, (src, dst) in enumerate(pairs)]
    for c in copies:
        c.start()
    for c in copies:
        c.wait()


def prepare_kernel(k, *refs):
    n = 7
    far, refs = refs[:n], refs[n:]
    if k:
        before, refs = refs[0], refs[2:]
    out_q, out_k, held, sems = refs[0], refs[1], refs[2 : 2 + n], refs[2 + n]

    if k:
        @pl.when(jnp.logical_not(turn(k)))
        def _():
            out_k[...] = before[...]

    @pl.when(turn(k))
    def _():
        fetch(zip(far, held), sems)
        keys, gain, bias, pos, freq, w, q = held
        angle = freq[...] * pos[...].astype(jnp.float32)
        cosine, sine = jnp.cos(angle), jnp.sin(angle)
        out_k[...] = turned(keys[...], gain[...], bias[...], cosine, sine)
        turn_queries(q, w, cosine, sine, out_q)


def prepare(k, sources, before=()):
    n = len(sources)
    return pl.pallas_call(
        functools.partial(prepare_kernel, k),
        out_shape=(pltpu.VMEM((DH + 16, QT), jnp.bfloat16), pltpu.VMEM((ROWS, DH), jnp.bfloat16)),
        in_specs=[ANY] * n + [VMEM] * len(before),
        out_specs=(VMEM, VMEM),
        input_output_aliases={n + 1: 0} if k else {},
        scratch_shapes=[pltpu.VMEM(x.shape, x.dtype) for x in sources] + [pltpu.SemaphoreType.DMA((n,))],
    )(*sources, *[near(x) for x in before])


def pack_kernel(own_0, own_13, own_2, from_0, near_by, far_off, out):
    group = lax.axis_index("zh")
    own = jnp.where(group == 0, own_0[...], jnp.where(group == 2, own_2[...], own_13[...]))
    last = jnp.where(group == 1, from_0[...], near_by[...])
    for slot, x in enumerate((own, last, far_off[...])):
        for d in range(PEERS):
            out[d, slot] = x


def score_kernel(q0, q1, q2, q3, k, pos, out):
    _, first, group, z = where_am_i()
    row = lax.broadcasted_iota(jnp.int32, (ROWS, 1), 0) + first
    doc = row - column(pos[...].astype(jnp.float32), ROWS, 0).astype(jnp.int32)

    def one(slot, start, n):
        peers = slice(start // ROWS, (start + n) // ROWS)
        kk = k[peers, slot].reshape(n, DH)
        acc = jnp.zeros((n, DH), jnp.float32)
        for q in (q0, q1, q2, q3):
            w = q[DH : DH + 1, :].astype(jnp.float32)
            for c in range(0, QT, 1024):
                s = jnp.dot(kk, q[:DH, c : c + 1024], preferred_element_type=jnp.float32)
                for p in range(0, 1024, DH):
                    acc = acc + jnp.maximum(s[:, p : p + DH], 0.0) * w[:, c + p : c + p + DH]
        acc = acc.T
        acc = acc[:ROWS] + acc[ROWS:]
        key = plane_start(slot) + start + lax.broadcasted_iota(jnp.int32, (1, n), 1)
        seen = (key >= doc) & (key <= row)
        out[:, slot, :, start : start + n] = (
            jnp.where(seen, acc * SCALE, 0.0).astype(jnp.bfloat16).reshape(4, SUB, n)
        )

    def plane_start(slot):
        return (group - slot) * GROUP + z * PLANE

    for start, n in ((0, 128), (128, 128), (256, 256)):
        reached = plane_start(0) + start < first + ROWS

        @pl.when(reached)
        def _():
            one(0, start, n)

        @pl.when(jnp.logical_not(reached))
        def _():
            out[:, 0, :, start : start + n] = jnp.zeros((4, SUB, n), jnp.bfloat16)

    for slot in range(1, SLOTS):
        live = (slot <= group) & (group < 3)

        @pl.when(live)
        def _():
            one(slot, 0, NK)

        @pl.when(jnp.logical_not(live))
        def _():
            out[:, slot] = jnp.zeros((4, SUB, NK), jnp.bfloat16)


def place_kernel(parts, out):
    head, _, group, z = where_am_i()
    out[...] = jnp.zeros_like(out)
    live = jnp.where(group == 3, 1, group + 1)
    for slot in range(SLOTS):
        @pl.when(slot < live)
        def _():
            for j in range(4):
                at = pl.multiple_of((group - slot) * GROUP + (z ^ head ^ j) * PLANE, PLANE)
                out[:, pl.ds(at, PLANE)] = parts[j, slot].astype(jnp.float32)


VMEM = pl.BlockSpec(memory_space=pltpu.VMEM)
ANY = pl.BlockSpec(memory_space=pl.ANY)


def call(kernel, shape, dtype, *args, inside=True):
    if inside:
        out = pltpu.VMEM(shape, dtype)
    else:
        out = jax.ShapeDtypeStruct(shape, dtype)
    return pl.pallas_call(kernel, out_shape=out, in_specs=[VMEM] * len(args), out_specs=VMEM)(*args)


def near(x):
    return pltpu.with_memory_space_constraint(x, pltpu.VMEM)


LINE = ("zh", "zl", "yh", "yl", "core")


def hop(src, dst, cross):
    def at(g, z, j):
        return (g * 4 + z) * 8 + j

    return [
        (at(src, z, j), at(dst, z ^ m if cross else z, j))
        for z in range(4) for j in range(8) for m in ((j & 3) ^ (j >> 2) * 2,)
    ]


NEAR = [[(x * 2 + h) * 2 + (t ^ h) for x in range(4) for h in range(2)] for t in range(2)]


def program(queries, keys, key_gain, key_bias, head_weights, positions):
    freq = jnp.asarray(yarn_frequencies(ROPE)[:, None])
    gain, bias = key_gain.reshape(1, DH), key_bias.reshape(1, DH)
    pos = positions.reshape(1, ROWS)
    weights = head_weights.T

    sources = (keys, gain, bias, pos, freq, weights, queries)

    q, mine = prepare(0, sources)
    own_0 = lax.ppermute(mine, LINE, hop(0, 0, True))
    from_0 = lax.ppermute(own_0, LINE, hop(0, 1, False))
    q, mine = prepare(1, sources, (mine, q))
    own_13 = lax.ppermute(mine, LINE, hop(1, 1, True) + hop(3, 3, True))
    far_off = lax.ppermute(from_0, LINE, hop(1, 2, False))
    q0, mine = prepare(2, sources, (mine, q))
    swap = [(0, 1), (1, 0)]
    q1 = lax.ppermute(q0, "yl", swap)
    near_by = lax.ppermute(own_13, LINE, hop(1, 2, False))
    own_2 = lax.ppermute(mine, LINE, hop(2, 2, True))
    q2 = lax.ppermute(q0, "core", swap)
    q3 = lax.ppermute(q1, "core", swap)

    sent = call(
        pack_kernel, (PEERS, SLOTS, ROWS, DH), jnp.bfloat16,
        near(own_0), near(own_13), near(own_2), near(from_0), near(near_by), near(far_off),
    )
    k_all = lax.all_to_all(
        sent, ("x", "yh", "yl"), 0, 0, axis_index_groups=NEAR, tiled=True
    )

    parts = call(
        score_kernel, (4, SLOTS, SUB, NK), jnp.bfloat16,
        near(q0), near(q1), near(q2), near(q3), near(k_all), near(pos),
    )
    parts = lax.all_to_all(parts, ("yl", "core"), 0, 0, tiled=True)
    return call(place_kernel, (SUB, 8192), jnp.float32, near(parts), inside=False)


def solution(mesh):
    names = ("zh", "zl", "x", "yh", "yl", "core")
    fine = Mesh(mesh.devices.reshape(4, 4, 4, 2, 2, 2), names)
    ctx, head = names[:4], names[4:]
    in_specs = (P(ctx, head), P(ctx, None), P(), P(), P(ctx, head), P(ctx))
    return jax.shard_map(program, mesh=fine, in_specs=in_specs, out_specs=P(names, None), check_vma=False)
```
